128 devices in a mesh: rows: 16 (over y_lo, x, core), snap: 8 (over z, y_hi).
Axes of the slice: x: 4, y: 4 (y_hi: 2, y_lo: 2; y = y_hi * 2 + y_lo), z: 4, core: 2. Of those that a mesh axis runs over, the one named last changes fastest.
Arguments:
- direct: bfloat16 [131072, 1024], P('rows', 'snap'), may hold values from -6 to 6
- adjoint: bfloat16 [131072, 1024], P('rows', 'snap'), may hold values from -6 to 6
- right_vectors: bfloat16 [1024, 256], replicated, may hold values from -0.1875 to 0.1875
- left_vectors: bfloat16 [1024, 256], replicated, may hold values from -0.1875 to 0.1875
- singular: float32 [256], replicated, may hold values from 0.25 to 4
Outputs:
- gram: float32 [1024, 1024], P('snap', 'rows')
- balancing: bfloat16 [131072, 256], P('rows', 'snap')
- adjoint_modes: bfloat16 [131072, 256], P('rows', 'snap')
The draws below stay inside these ranges and needn't reach their ends.
All inputs are finite; a program needn't handle non-finite values.
Results may differ from the reference program's by a relative error of at most 0.0045.
Values may be sent and summed in bfloat16 or wider, within the bound.
No kernel may reach another device: no remote copies, remote signals or barrier semaphores. Data moves between devices by JAX's collectives and lax.ppermute only.
A program may use at most 128 MiB of HBM per device.

```python
import math
import jax
import jax.numpy as jnp
from jax import lax

M = 1024
R = 256
NROWS = 131072


def strengthened(array, key, source, target, blocks, factor):
    def block_of(position):
        return (jnp.arange(array.shape[position]) // (array.shape[position] // blocks)).reshape((-1,) + (1,) * (array.ndim - 1 - position))

    first = jax.random.permutation(key, blocks)[block_of(target)]
    other_side = (block_of(target) + blocks // 2) % blocks
    return jnp.where((block_of(source) == first) | (block_of(source) == other_side), factor * array, array)


def shard_levels(stream_key, dims, pieces, low, high):
    level = 1.0
    for axis_at, shards_of in pieces:
        steps = jax.random.uniform(jax.random.fold_in(jax.random.fold_in(stream_key, 6), axis_at), (shards_of,), jnp.float32, low / len(pieces), high / len(pieces))
        level = level * jnp.repeat(jnp.exp(steps), dims[axis_at] // shards_of).reshape((-1,) + (1,) * (len(dims) - 1 - axis_at))
    return level


def scatter_about(key, shape, spread, most, pieces=(), dtype=jnp.bfloat16):
    values = spread * jax.random.normal(key, shape, jnp.float32)
    if pieces:
        values = values * shard_levels(key, shape, pieces, -0.22, 0.18)
    return jnp.clip(values, -most, most).astype(dtype)


def noise_with(own_key, extent, spread, reach, shards, heavy, kind=jnp.bfloat16):
    array = spread * jax.random.normal(own_key, extent, jnp.float32)
    if shards:
        array = array * shard_levels(own_key, extent, shards, -0.22, 0.18)
    return jnp.clip(strengthened(array, jax.random.fold_in(own_key, 3), *heavy), -reach, reach).astype(kind)


def setup_inputs(seed: int = 0) -> dict:
    seeds = jax.random.split(jax.random.key(seed), 6)
    direct = noise_with(seeds[0], (NROWS, M), 1.0, 6.0, ((0, 16), (1, 8)), (0, 1, 16, 2.0))
    adjoint = scatter_about(seeds[1], (NROWS, M), 1.0, 6.0, ((0, 16), (1, 8)))
    right_vectors = scatter_about(seeds[2], (M, R), M ** -0.5, 0.1875)
    left_vectors = scatter_about(seeds[3], (M, R), M ** -0.5, 0.1875)
    singular = jnp.clip(jnp.exp(jax.random.uniform(seeds[4], (R,), jnp.float32, math.log(0.25), math.log(4.0))), 0.25, 4.0)
    return {"direct": direct, "adjoint": adjoint, "right_vectors": right_vectors, "left_vectors": left_vectors, "singular": singular}


def reference(direct, adjoint, right_vectors, left_vectors, singular):
    nrows = direct.shape[0]
    cross = lax.dot_general(adjoint, direct, (((0,), (0,)), ((), ())), preferred_element_type=jnp.float32)
    gram = cross / jnp.sqrt(jnp.float32(nrows))
    weights = lax.rsqrt(singular.astype(jnp.float32))
    balancing = (jnp.dot(direct, right_vectors, preferred_element_type=jnp.float32) * weights).astype(jnp.bfloat16)
    adjoint_modes = (jnp.dot(adjoint, left_vectors, preferred_element_type=jnp.float32) * weights).astype(jnp.bfloat16)
    return (gram, balancing, adjoint_modes)
```

```python
import jax
import jax.numpy as jnp
from jax import lax
from jax.sharding import PartitionSpec as P


def swap(block, pairs):
    return lax.ppermute(block, ("rows", "snap"), pairs)


def on_device(direct, adjoint, right_vectors, left_vectors, singular):
    nrow, nsnap = lax.axis_size("rows"), lax.axis_size("snap")
    rows, cols = direct.shape
    part = rows // nsnap
    m = cols * nsnap
    r = right_vectors.shape[1]
    width = m // nrow
    bf, f32 = jnp.bfloat16, jnp.float32

    def turned(a):
        return lax.all_to_all(a.reshape(nsnap, part, cols), "snap", 0, 0, tiled=True)

    x8 = turned(direct)
    y8 = turned(adjoint)
    x = x8.transpose(1, 0, 2).reshape(part, m)
    y = y8.transpose(1, 0, 2).reshape(part, m)
    weights = lax.rsqrt(singular)

    def modes(a, v):
        t = lax.dot_general(v, a, (((0,), (1,)), ((), ())), preferred_element_type=f32)
        t = (t * weights[:, None]).astype(bf).reshape(nsnap, r // nsnap, part)
        t = lax.all_to_all(t, "snap", 0, 0, tiled=True)
        return t.transpose(0, 2, 1).reshape(rows, r // nsnap)

    g = lax.dot_general(x, y, (((0,), (0,)), ((), ())), preferred_element_type=f32)
    g = g * (1.0 / jnp.sqrt(f32(rows * nrow)))
    g = g.reshape(2, nrow // 4, 2, width, m)
    ri = lax.axis_index("rows")
    core = ri % 2
    keep = lax.dynamic_index_in_dim(g, core, 2, keepdims=False)
    give = lax.dynamic_index_in_dim(g, 1 - core, 2, keepdims=False).astype(bf)
    pairs = [(i, i ^ 1) for i in range(nrow)]
    g = keep + lax.ppermute(give, "rows", pairs).astype(f32)
    groups = [[yl * (nrow // 2) + xx * 2 + c for xx in range(nrow // 4)] for yl in range(2) for c in range(2)]
    h = g.astype(bf).transpose(1, 0, 2, 3)
    h = lax.all_to_all(h, "rows", 0, 0, axis_index_groups=groups, tiled=True)
    h = jnp.sum(h.astype(f32), axis=0)
    ylo = ri // (nrow // 2)
    keep = lax.dynamic_index_in_dim(h, ylo, 0, keepdims=False)
    give = lax.dynamic_index_in_dim(h, 1 - ylo, 0, keepdims=False).astype(bf)
    pairs = [(i, (i + nrow // 2) % nrow) for i in range(nrow)]
    h = keep + lax.ppermute(give, "rows", pairs).astype(f32)
    h = h.astype(bf).reshape(width, nsnap, cols).transpose(1, 0, 2)
    h = lax.all_to_all(h, "snap", 0, 0, tiled=True)
    gram = jnp.sum(h.astype(f32), axis=0).T
    return gram, modes(x, right_vectors), modes(y, left_vectors)


def solution(mesh):
    return jax.shard_map(
        on_device,
        mesh=mesh,
        in_specs=(P("rows", "snap"), P("rows", "snap"), P(), P(), P()),
        out_specs=(P("snap", "rows"), P("rows", "snap"), P("rows", "snap")),
        check_vma=False,
    )
```
